32 devices in a mesh: node: 4 (over y, core), rep: 8 (over z, x).
Axes of the slice: x: 2, y: 2, z: 4, core: 2. Of those that a mesh axis runs over, the one named last changes fastest.
Arguments:
- tokens: bfloat16 [8192, 2048], P(('node', 'rep')), may hold values from -60 to 60
- cotangent: bfloat16 [8192, 512], P(('node', 'rep')), may hold values from -6 to 6
- value_weight: bfloat16 [2048, 512], P('node'), may hold values from -0.25 to 0.25
Outputs:
- input_grad: bfloat16 [8192, 2048], P(('node', 'rep'))
- update: float32 [2048, 512], P('node')
The draws below stay inside these ranges and needn't reach their ends.
All inputs are finite; a program needn't handle non-finite values.
Results may differ from the reference program's by a relative error of at most 0.025.
Values may be sent and summed in bfloat16 or wider, within the bound.
A program may use at most 64 MiB of HBM per device.

```python
import math
import jax
import jax.numpy as jnp
from jax import lax

DIN = 2048
KVH = 4
HD = 128
NS_ITERS = 5
TOK_DEV = 256
CV = 512
TOKENS = 8192
N_NODE = 4


def draw_tokens(key, part):
    key_values = jax.random.fold_in(key, 11)
    key_rough = jax.random.fold_in(key, 12)
    key_pair = jax.random.fold_in(key, 13)
    columns = jnp.arange(DIN, dtype=jnp.float32) / (DIN - 1)
    rough = jnp.exp(jax.random.uniform(key_rough, (DIN,), jnp.float32, jnp.log(0.7), jnp.log(1.4)))
    values = jnp.clip(jax.random.normal(key_values, (TOKENS, DIN), jnp.float32), -6.0, 6.0)
    rise = 3.0 ** columns
    offset = jax.random.randint(key_pair, (), 0, N_NODE)
    row_block = jnp.arange(TOKENS, dtype=jnp.int32) // TOK_DEV
    col_block = jnp.arange(DIN, dtype=jnp.int32) // (DIN // N_NODE)
    paired = ((row_block + offset) % N_NODE)[:, None] == col_block[None, :]
    spike = jnp.where(paired, 3.0, 1.0).astype(jnp.float32)
    return (values * spike * (rise * rough)[None, :]).astype(jnp.bfloat16)


def shard_levels(own_key, dims, pieces, smallest, high):
    loudness, own = 1.0, jax.random.fold_in(own_key, 6)
    for position, shards_of in pieces:
        draws = jnp.exp(jax.random.uniform(jax.random.fold_in(own, position), (shards_of,), jnp.float32, smallest / len(pieces), high / len(pieces)))
        loudness = loudness * jnp.repeat(draws, dims[position] // shards_of).reshape([-1 if axis == position else 1 for axis in range(len(dims))])
    return loudness


def noise(key, extent, deviation, most, split=(), kind=jnp.bfloat16):
    drawn = jax.random.normal(key, extent, jnp.float32) * deviation
    if len(split) > 0:
        drawn = shard_levels(key, extent, split, -0.22, 0.18) * drawn
    return jnp.clip(drawn, min=-most, max=most).astype(kind)


def setup_inputs(seed: int = 0) -> dict:
    seeds = jax.random.split(jax.random.key(seed), 4)
    tokens = draw_tokens(jax.random.fold_in(seeds[3], 71), 0)
    cotangent = noise(seeds[1], (TOKENS, CV), 1.0, 6.0, ((0, 32),))
    value_weight = noise(seeds[2], (DIN, CV), CV ** -0.5, 0.25, ((0, 4),))
    return {"tokens": tokens, "cotangent": cotangent, "value_weight": value_weight}


coef_a = 3.4445
coef_b = -4.775
coef_c = 2.0315
epsilon = 1e-07

def block_term(total, pair):
    rows_x, rows_c = pair
    term = jnp.einsum('td,tc->dc', rows_x.astype(jnp.float32), rows_c.astype(jnp.float32), precision=lax.Precision.HIGHEST)
    rounded = lax.optimization_barrier(term.astype(jnp.bfloat16))
    return (total + rounded.astype(jnp.float32), None)

def reference(tokens, cotangent, value_weight):
    width = cotangent.shape[1]
    input_grad = jnp.dot(cotangent, value_weight.T, preferred_element_type=jnp.float32).astype(jnp.bfloat16)
    blocks_x = tokens.reshape(-1, TOK_DEV, DIN)
    blocks_c = cotangent.reshape(-1, TOK_DEV, width)
    gradient, unused = lax.scan(block_term, jnp.zeros((DIN, width), jnp.float32), (blocks_x, blocks_c))
    blocks = gradient.reshape(DIN, KVH, HD)
    norms = jnp.sqrt(lax.optimization_barrier(jnp.sum(blocks * blocks, axis=(0, 2))))
    iterate = blocks / (norms[None, :, None] + epsilon)
    for step in range(NS_ITERS):
        gram = jnp.einsum('rhi,rhj->hij', iterate, iterate, precision=lax.Precision.HIGHEST)
        poly = coef_b * gram + coef_c * jnp.einsum('hij,hjk->hik', gram, gram, precision=lax.Precision.HIGHEST)
        iterate = coef_a * iterate + jnp.einsum('rhi,hij->rhj', iterate, poly, precision=lax.Precision.HIGHEST)
    update = 0.2 * math.sqrt(DIN) * iterate.reshape(DIN, width)
    return (input_grad, update)
```

```python
import functools
import math

import jax
import jax.numpy as jnp
from jax import lax
from jax.experimental import pallas as pl
from jax.experimental.pallas import tpu as pltpu
from jax.sharding import PartitionSpec as P

HD = 128
NS_ITERS = 5
WPARTS = 8
W_EARLY = 1
ORDER = ("z0", "z1", "z2", "r0", "z3", "f1", "r1", "f2", "r2", "f3", "l0", "r3", "l1", "g0", "l2", "g1", "e0", "l3", "g2", "e1", "g3", "w", "e2", "e3", "i", "o0", "o1", "o2", "o3")

coef_a = 3.4445
coef_b = -4.775
coef_c = 2.0315
epsilon = 1e-07

MESH = pl.DeviceIdType.MESH
F32, BF16 = jnp.float32, jnp.bfloat16


def mm_t(a, b):
    return lax.dot_general(a, b, (((0,), (0,)), ((), ())), preferred_element_type=F32)


def parts_of(a):
    hi = a.astype(BF16)
    lo = (a - hi.astype(F32)).astype(BF16)
    return hi, lo


def left_form(a):
    return jnp.concatenate(parts_of(a), axis=1)


def right_form(b):
    row = jnp.concatenate(parts_of(b), axis=1)
    return jnp.concatenate([row, row], axis=0)


def product(left, right):
    n = right.shape[1] // 2
    wide = jnp.dot(left, right, preferred_element_type=F32)
    return wide[:, :n] + wide[:, n:]


def kernel(cfg, tok_hbm, cot_hbm, w_hbm, igbuf, rows_ref, form_ref, tok_ref, cot_ref, w_ref, tokx, cotx, wall, acc, send1, recv1, send2,
           recv2, zsend, zrecv, grad, early, gram_own, gram_in, lsem, ssem, rsem):
    width, heads, zs = cfg
    din = tok_ref.shape[1]
    block = din // 4
    half, quarter = block // 2, block // 4
    wpart = block // WPARTS

    node, rep = lax.axis_index("node"), lax.axis_index("rep")
    y, c = node // 2, node % 2
    z, x = rep // 2, rep % 2
    partner = (y * 2 + 1 - c, rep)
    y_peer = ((1 - y) * 2 + c, rep)
    x_peer = (node, z * 2 + 1 - x)
    z_others = [(node, lax.rem(z + d, zs) * 2 + x) for d in range(1, zs)]
    bits = [(y, x), (x, y)]
    towards = [(y_peer, x_peer), (x_peer, y_peer)]
    roots = [zs // 2 - 1 + p for p in range(2)]

    names = {}

    def sem(of, name):
        return of.at[names.setdefault((id(of), name), sum(1 for key in names if key[0] == id(of)))]

    def copy_to(src, dst, peer, out, into):
        return pltpu.make_async_remote_copy(src_ref=src, dst_ref=dst, send_sem=sem(ssem, out), recv_sem=sem(rsem, into),
                                            device_id=peer, device_id_type=MESH)

    def remote(src, dst, peer, out, into):
        cp = copy_to(src, dst, peer, out, into)
        cp.start()
        return cp

    def received(ref, into):
        pltpu.make_async_remote_copy(src_ref=ref, dst_ref=ref, send_sem=ssem.at[0], recv_sem=sem(rsem, into),
                                     device_id=partner, device_id_type=MESH).wait_recv()

    def sent(ref, out):
        pltpu.make_async_remote_copy(src_ref=ref, dst_ref=ref, send_sem=sem(ssem, out), recv_sem=rsem.at[0],
                                     device_id=partner, device_id_type=MESH).wait_send()

    def start_of(p, i):
        b0, b1 = bits[p]
        h = 1 - b0 if i < 2 else b0
        q = 1 - b1 if i % 2 == 0 else b1
        return h * half + q * quarter

    def quarter_rows(p, i):
        return pl.ds(pl.multiple_of(start_of(p, i), quarter), quarter)

    def col(p, core, i):
        return pl.ds(pl.multiple_of((2 * p + core) * block + start_of(p, i), quarter), quarter)

    own_w = pl.ds(pl.multiple_of(node * block, block), block)

    pairs = ((cot_hbm, cot_ref), (tok_hbm, tok_ref), (w_hbm, w_ref))
    loads = [pltpu.make_async_copy(src, dst, lsem.at[i]) for i, (src, dst) in enumerate(pairs)]
    for cp in loads:
        cp.start()

    barrier = pltpu.get_barrier_semaphore()
    peers = [partner, y_peer, x_peer] + z_others
    for peer in peers:
        pl.semaphore_signal(barrier, inc=1, device_id=peer, device_id_type=MESH)
    pl.semaphore_wait(barrier, len(peers))

    for cp in loads[:2]:
        cp.wait()
    remote(cot_ref, cotx, partner, "cot", "cot")
    for i in range(4):
        for p in range(2):
            remote(tok_ref.at[:, col(p, 1 - c, i)], tokx.at[p, :, quarter_rows(p, i)], partner, "tok", f"tok{i}")
    loads[2].wait()

    def w_part(n, side, i):
        return pl.ds(pl.multiple_of(n * block + side * half + i * wpart, wpart), wpart)

    def send_w(i):
        rows = pl.ds(pl.multiple_of(x * half + i * wpart, wpart), wpart)
        remote(w_ref.at[rows], wall.at[w_part(node, x, i)], y_peer, "wy", f"wy{i}")

    def relay_w(i):
        rows = w_part((1 - y) * 2 + c, x, i)
        received(wall.at[rows], f"wy{i}")
        remote(wall.at[rows], wall.at[rows], x_peer, "wx", "wx")

    nw = WPARTS // 2
    for i in range(W_EARLY):
        send_w(i)

    def both(i, first, other):
        pair = jnp.concatenate([first(p, i) for p in range(2)], axis=1)
        return mm_t(pair, other[...])

    def own_tok(p, i):
        return tok_ref[:, col(p, c, i)]

    def their_tok(p, i):
        return tokx[p, :, quarter_rows(p, i)]

    for i in range(4):
        acc[i] = both(i, own_tok, cot_ref)

    def chip_sum(i):
        if i == 0:
            received(cotx, "cot")
        received(tokx.at[0, :, pl.ds(0, 2 * quarter)], f"tok{i}")
        return acc[i] + both(i, their_tok, cotx)

    def cs(s):
        return slice(s * HD, (s + 1) * HD)

    def pr(p):
        return slice(p * quarter, (p + 1) * quarter)

    st1 = {}
    for i in range(2):
        value = chip_sum(i).astype(BF16)
        for s in range(heads):
            for p in range(2):
                send1[i, p, s] = value[pr(p), cs(s)]
                st1[i, p, s] = copy_to(send1.at[i, p, s], recv1.at[i, p, s], towards[p][0], "first", f"first{i}{s}")
                if i == 0 or s == 0:
                    st1[i, p, s].start()
    remote(w_ref, wall.at[own_w], partner, "wp", "wp")
    for i in range(2, 4):
        acc[i] = chip_sum(i)

    to_z, bcast, sg2, sg1 = {}, {}, {}, {}

    def second(s):
        received(recv1.at[0, :, s], f"first0{s}")
        for p in range(2):
            send2[p, s] = (acc[2, pr(p), cs(s)] + recv1[0, p, s].astype(F32)).astype(BF16)
            remote(send2.at[p, s], recv2.at[p, s], towards[p][1], "second", f"second{s}")
        if s + 1 < heads:
            for p in range(2):
                st1[1, p, s + 1].start()

    def to_root(s):
        received(recv1.at[1, :, s], f"first1{s}")
        received(recv2.at[:, s], f"second{s}")
        for p in range(2):
            total = acc[3, pr(p), cs(s)] + recv1[1, p, s].astype(F32) + recv2[p, s].astype(F32)
            slot = lax.rem(z + 2 * zs - roots[p] - 1, zs)
            to_z[p, s] = copy_to(zsend.at[p, s], zrecv.at[s, slot], (node, roots[p] * 2 + x), f"z{p}", f"z{s}")

            @pl.when(z == roots[p])
            def _():
                acc[3, pr(p), cs(s)] = total

            @pl.when(z != roots[p])
            def _():
                zsend[p, s] = total.astype(BF16)
                to_z[p, s].start()

            mine = quarter_rows(p, 3)
            here = grad.at[p, s, mine]
            bcast[p, s] = [copy_to(here, here, (node, (roots[p] + d) % zs * 2 + x), "down", f"{('first1', 'second')[p]}{s}")
                           for d in range(1, zs)]
            sg1[p, s] = copy_to(here, here, towards[p][0], "gather", f"tok{s}")
            sg2[p, s] = copy_to(here, here, towards[p][1], "gather", f"first0{s}")

    def spread(p, s):
        sg2[p, s].start()
        sg1[p, s].start()

    def from_root(s):
        for p in range(2):
            @pl.when(z == roots[p])
            def _():
                total = acc[3, pr(p), cs(s)]
                received(zrecv.at[s], f"z{s}")
                for d in range(zs - 1):
                    total = total + zrecv[s, d].astype(F32)
                grad[p, s, quarter_rows(p, 3)] = total.astype(BF16)
                for cp in bcast[p, s]:
                    cp.start()
                spread(p, s)

    def at_leaf(s):
        for p in range(2):
            @pl.when(z != roots[p])
            def _():
                bcast[p, s][0].wait_recv()
                spread(p, s)

    def last_gather(s):
        received(grad.at[:, s, pl.ds(0, quarter)], f"first0{s}")
        for p in range(2):
            there = grad.at[p, s, quarter_rows(p, 2)]
            remote(there, there, towards[p][0], "gather", f"tok{s}")

    def input_rows(n, rows_of_w):
        rows = pl.ds(pl.multiple_of(n * block, block), block)
        out = lax.dot_general(cot_ref[...], rows_of_w, (((1,), (1,)), ((), ())), preferred_element_type=F32)
        igbuf[:, rows] = out.astype(BF16)

    def gathered(n):
        return wall[pl.ds(pl.multiple_of(n * block, block), block), :]

    def gram_of(h, p, bit):
        rows = pl.ds(pl.multiple_of(bit * half, half), half)
        g = grad[p, h, rows]
        return mm_t(g, g)

    for s in range(heads):
        second(s)
    for i in range(W_EARLY):
        relay_w(i)
    for i in range(W_EARLY, nw):
        send_w(i)
    input_rows(node, w_ref[...])
    received(w_ref, "wp")
    input_rows(y * 2 + 1 - c, gathered(y * 2 + 1 - c))

    def swap_w():
        received(wall.at[pl.ds(0, half)], "wx")
        y_w = pl.ds(pl.multiple_of(((1 - y) * 2 + c) * block, block), block)
        remote(wall.at[y_w], wall.at[y_w], partner, "wp", "wf")

    def finish_input():
        input_rows((1 - y) * 2 + c, gathered((1 - y) * 2 + c))
        received(w_ref, "wf")
        input_rows((1 - y) * 2 + 1 - c, gathered((1 - y) * 2 + 1 - c))

    def early_gram(s):
        early[s] = gram_of(s, 0, y) + gram_of(s, 1, x)

    def own_gram(s):
        received(grad.at[:, s, pl.ds(0, half)], f"tok{s}")
        gram_own[s] = early[s] + (gram_of(s, 0, 1 - y) + gram_of(s, 1, 1 - x))
        remote(gram_own.at[s], gram_in.at[s], partner, "gram", "gram")

    steps = {"z": to_root, "r": from_root, "l": at_leaf, "g": last_gather, "e": early_gram, "o": own_gram, "f": relay_w}
    extra = {"w": swap_w, "i": finish_input}
    for word in ORDER:
        if word in extra:
            extra[word]()
        else:
            steps[word[0]](int(word[1:]))

    rows_ref[...] = grad[y]
    received(gram_in, "gram")

    ii = lax.broadcasted_iota(jnp.int32, (HD, HD), 0)
    jj = lax.broadcasted_iota(jnp.int32, (HD, HD), 1)
    eye = (ii == jj).astype(F32)
    grams, totals, scales = [], [None] * heads, []
    for h in range(heads):
        raw = gram_own[h] + gram_in[h]
        squares = jnp.sum(jnp.sum(raw * eye, axis=1, keepdims=True), axis=0, keepdims=True)
        inverse = 1.0 / (jnp.sqrt(squares) + epsilon)
        scales.append(inverse)
        grams.append(raw * inverse * inverse)
    for step in range(NS_ITERS):
        rights = [right_form(g) for g in grams]
        squared = [product(left_form(g), r) for g, r in zip(grams, rights)]
        factors = [coef_a * eye + coef_b * g + coef_c * q for g, q in zip(grams, squared)]
        forms = [right_form(f) for f in factors]
        if step + 1 < NS_ITERS:
            halfway = [product(left_form(g), f) for g, f in zip(grams, forms)]
        if step == 0:
            totals = factors
        else:
            totals = [product(left_form(t), f) for t, f in zip(totals, forms)]
        if step + 1 < NS_ITERS:
            grams = [product(left_form(g), f) for g, f in zip(halfway, forms)]

    for h in range(heads):
        scaled = totals[h] * (scales[h] * (0.2 * math.sqrt(din)))
        form_ref[h] = jnp.concatenate(parts_of(scaled), axis=1)
    sent(cotx, "cot")
    sent(tokx, "tok")
    sent(send1, "first")
    sent(send2, "second")
    sent(wall.at[pl.ds(0, half)], "wy")
    sent(wall.at[pl.ds(0, half)], "wx")
    sent(wall.at[pl.ds(0, 2 * block)], "wp")
    sent(grad.at[:, :, pl.ds(0, 3 * quarter)], "gather")
    sent(gram_own, "gram")
    for p in range(2):
        @pl.when(z == roots[p])
        def _():
            sent(grad.at[0, :, pl.ds(0, 3 * quarter)], "down")

        @pl.when(z != roots[p])
        def _():
            sent(zsend.at[p], f"z{p}")


def finish(ig_ref, rows_ref, form_ref, ig_out, up_out, upbuf, sems):
    heads = form_ref.shape[0]
    step = upbuf.shape[0] // 4
    copies = [pltpu.make_async_copy(ig_ref, ig_out, sems.at[0])]
    copies[0].start()
    for i in range(4):
        part = pl.ds(i * step, step)
        for h in range(heads):
            upbuf[part, pl.ds(h * HD, HD)] = product(rows_ref[h, part], form_ref[h])
        copies.append(pltpu.make_async_copy(upbuf.at[part], up_out.at[part], sems.at[i + 1]))
        copies[-1].start()
    for cp in copies:
        cp.wait()


def fused(tokens, cotangent, value_weight, zs):
    tok, din = tokens.shape
    width = cotangent.shape[1]
    heads = width // HD
    block = din // 4
    quarter = block // 4
    nsend = 12
    nrecv = 1 + 4 + 4 * heads + WPARTS // 2 + 4
    vm, dma = pltpu.VMEM, pltpu.SemaphoreType.DMA
    held = pl.pallas_call(
        functools.partial(kernel, (width, heads, zs)),
        out_shape=(
            jax.ShapeDtypeStruct((tok, din), BF16),
            jax.ShapeDtypeStruct((heads, block, HD), BF16),
            jax.ShapeDtypeStruct((heads, HD, 2 * HD), BF16),
        ),
        in_specs=[pl.BlockSpec(memory_space=pl.ANY)] * 3,
        out_specs=(pl.BlockSpec(memory_space=pltpu.VMEM),) * 3,
        scratch_shapes=[
            vm((tok, din), BF16),
            vm((tok, width), BF16),
            vm((block, width), BF16),
            vm((2, tok, block), BF16),
            vm((tok, width), BF16),
            vm((din, width), BF16),
            vm((4, 2 * quarter, width), F32),
            vm((2, 2, heads, quarter, HD), BF16),
            vm((2, 2, heads, quarter, HD), BF16),
            vm((2, heads, quarter, HD), BF16),
            vm((2, heads, quarter, HD), BF16),
            vm((2, heads, quarter, HD), BF16),
            vm((heads, zs - 1, quarter, HD), BF16),
            vm((2, heads, block, HD), BF16),
            vm((heads, HD, HD), F32),
            vm((heads, HD, HD), F32),
            vm((heads, HD, HD), F32),
            dma((3,)),
            dma((nsend,)),
            dma((nrecv,)),
        ],
        compiler_params=pltpu.CompilerParams(collective_id=0, has_side_effects=True, vmem_limit_bytes=24 * 1024 * 1024),
    )(*(pltpu.with_memory_space_constraint(a, pltpu.HBM) for a in (tokens, cotangent, value_weight)))
    return pl.pallas_call(
        finish,
        out_shape=(jax.ShapeDtypeStruct((tok, din), BF16), jax.ShapeDtypeStruct((block, width), F32)),
        in_specs=[pl.BlockSpec(memory_space=pltpu.VMEM)] * 3,
        out_specs=(pl.BlockSpec(memory_space=pltpu.HBM),) * 2,
        scratch_shapes=[vm((block, width), F32), pltpu.SemaphoreType.DMA((5,))],
        compiler_params=pltpu.CompilerParams(vmem_limit_bytes=8 * 1024 * 1024),
    )(*held)


def general(tokens, cotangent, value_weight):
    width = value_weight.shape[1]
    din = tokens.shape[1]
    local_rows = value_weight.shape[0]
    heads = width // HD
    input_grad = lax.dot_general(
        cotangent,
        lax.all_gather(value_weight, "node", axis=0, tiled=True),
        (((1,), (1,)), ((), ())),
        preferred_element_type=F32,
    ).astype(BF16)
    partial_rows = lax.psum_scatter(
        lax.dot_general(tokens, cotangent, (((0,), (0,)), ((), ())), preferred_element_type=F32).astype(BF16),
        "node",
        scatter_dimension=0,
        tiled=True,
    ).astype(F32)
    gradient = lax.psum(partial_rows, "rep")
    blocks = gradient.reshape(local_rows, heads, HD)
    exact = functools.partial(jnp.einsum, precision=lax.Precision.HIGHEST)
    gram_raw = lax.psum(exact("rhi,rhj->hij", blocks, blocks), "node")
    divisor = jnp.sqrt(jnp.einsum("hii->h", gram_raw)) + epsilon
    gram = gram_raw / (divisor * divisor)[:, None, None]
    identity = jnp.broadcast_to(jnp.eye(HD, dtype=F32), (heads, HD, HD))
    total = identity
    for step in range(NS_ITERS):
        factor = coef_a * identity + coef_b * gram + coef_c * exact("hij,hjk->hik", gram, gram)
        total = exact("hij,hjk->hik", total, factor)
        if step + 1 < NS_ITERS:
            gram = exact("hji,hjk->hik", factor, exact("hij,hjk->hik", gram, factor))
    iterate = exact("rhi,hij->rhj", blocks / divisor[None, :, None], total)
    return input_grad, 0.2 * math.sqrt(din) * iterate.reshape(local_rows, width)


def solution(mesh):
    nodes, reps = mesh.shape["node"], mesh.shape["rep"]

    def per_device(tokens, cotangent, value_weight):
        zs = reps // 2
        fits = nodes == 4 and reps == 8 and tokens.shape[1] % (nodes * 4 * HD) == 0 and value_weight.shape[1] == 4 * HD
        if fits:
            return fused(tokens, cotangent, value_weight, zs)
        return general(tokens, cotangent, value_weight)

    return jax.shard_map(
        per_device,
        mesh=mesh,
        in_specs=(P(("node", "rep"), None), P(("node", "rep"), None), P("node", None)),
        out_specs=(P(("node", "rep"), None), P("node", None)),
        check_vma=False,
    )
```

```python
import functools
import math

import jax
import jax.numpy as jnp
from jax import lax
from jax.experimental import pallas as pl
from jax.experimental.pallas import tpu as pltpu
from jax.sharding import PartitionSpec as P

HD = 128
NS_ITERS = 5
WPARTS = 8
PIECES = 2
AHEAD = 2
SWAP_AT = 3
ORDER = (
    "z0", "z1", "z2", "z3", "f1", "z4", "z5", "r0", "z6", "r1", "z7", "r2", "r3", "l0", "r4", "f2",
    "l1", "r5", "l2", "r6", "l3", "r7", "g0", "l4", "g1", "l5", "g2", "e0", "l6", "l7", "g3", "g4",
    "e1", "g5", "g6", "e2", "g7", "w", "e3", "i", "o0", "o1", "o2", "o3",
)

coef_a = 3.4445
coef_b = -4.775
coef_c = 2.0315
epsilon = 1e-07

MESH = pl.DeviceIdType.MESH
F32, BF16 = jnp.float32, jnp.bfloat16


def mm_t(a, b):
    return lax.dot_general(a, b, (((0,), (0,)), ((), ())), preferred_element_type=F32)


def parts_of(a):
    hi = a.astype(BF16)
    lo = (a - hi.astype(F32)).astype(BF16)
    return hi, lo


def left_form(a):
    return jnp.concatenate(parts_of(a), axis=1)


def right_form(b):
    row = jnp.concatenate(parts_of(b), axis=1)
    return jnp.concatenate([row, row], axis=0)


def product(left, right):
    n = right.shape[1] // 2
    wide = jnp.dot(left, right, preferred_element_type=F32)
    return wide[:, :n] + wide[:, n:]


def kernel(cfg, tok_hbm, cot_hbm, w_hbm, igbuf, rows_ref, form_ref, tok_ref, cot_ref, w_ref, tokx, cotx, wall, acc, send1, recv1, send2,
           recv2, zsend, zrecv, grad, early, gram_own, gram_in, lsem, ssem, rsem):
    width, heads, zs = cfg
    din = tok_ref.shape[1]
    block = din // 4
    half, quarter = block // 2, block // 4
    wpart = block // WPARTS
    chunks = heads * PIECES
    rows_c = quarter // PIECES

    node, rep = lax.axis_index("node"), lax.axis_index("rep")
    y, c = node // 2, node % 2
    z, x = rep // 2, rep % 2
    partner = (y * 2 + 1 - c, rep)
    y_peer = ((1 - y) * 2 + c, rep)
    x_peer = (node, z * 2 + 1 - x)
    z_others = [(node, lax.rem(z + d, zs) * 2 + x) for d in range(1, zs)]
    bits = [(y, x), (x, y)]
    towards = [(y_peer, x_peer), (x_peer, y_peer)]
    roots = [zs // 2 - 1 + p for p in range(2)]

    names = {}

    def sem(of, name):
        return of.at[names.setdefault((id(of), name), sum(1 for key in names if key[0] == id(of)))]

    def copy_to(src, dst, peer, out, into):
        return pltpu.make_async_remote_copy(src_ref=src, dst_ref=dst, send_sem=sem(ssem, out), recv_sem=sem(rsem, into),
                                            device_id=peer, device_id_type=MESH)

    def remote(src, dst, peer, out, into):
        cp = copy_to(src, dst, peer, out, into)
        cp.start()
        return cp

    def received(ref, into):
        pltpu.make_async_remote_copy(src_ref=ref, dst_ref=ref, send_sem=ssem.at[0], recv_sem=sem(rsem, into),
                                     device_id=partner, device_id_type=MESH).wait_recv()

    def sent(ref, out):
        pltpu.make_async_remote_copy(src_ref=ref, dst_ref=ref, send_sem=sem(ssem, out), recv_sem=rsem.at[0],
                                     device_id=partner, device_id_type=MESH).wait_send()

    def start_of(p, i):
        b0, b1 = bits[p]
        h = 1 - b0 if i < 2 else b0
        q = 1 - b1 if i % 2 == 0 else b1
        return h * half + q * quarter

    def chunk_rows(p, i, t):
        return pl.ds(pl.multiple_of(start_of(p, i) + t % PIECES * rows_c, rows_c), rows_c)

    def quarter_rows(p, i):
        return pl.ds(pl.multiple_of(start_of(p, i), quarter), quarter)

    def col(p, core, i):
        return pl.ds(pl.multiple_of((2 * p + core) * block + start_of(p, i), quarter), quarter)

    own_w = pl.ds(pl.multiple_of(node * block, block), block)

    pairs = ((cot_hbm, cot_ref), (tok_hbm, tok_ref), (w_hbm, w_ref))
    loads = [pltpu.make_async_copy(src, dst, lsem.at[i]) for i, (src, dst) in enumerate(pairs)]
    for cp in loads:
        cp.start()

    barrier = pltpu.get_barrier_semaphore()
    peers = [partner, y_peer, x_peer] + z_others
    for peer in peers:
        pl.semaphore_signal(barrier, inc=1, device_id=peer, device_id_type=MESH)
    pl.semaphore_wait(barrier, len(peers))

    for cp in loads[:2]:
        cp.wait()
    remote(cot_ref, cotx, partner, "cot", "cot")
    for i in range(4):
        for p in range(2):
            remote(tok_ref.at[:, col(p, 1 - c, i)], tokx.at[p, :, quarter_rows(p, i)], partner, "tok", f"tok{i}")
    loads[2].wait()

    even = lax.rem(z, 2)
    z_pair = (node, (z + 1 - 2 * even) * 2 + x)
    w_at = [even, 1 - even, 2, 3]
    other = (1 - y) * 2 + c

    def w_rows(base, i, side):
        return pl.ds(pl.multiple_of(base + side * half + w_at[i] * wpart, wpart), wpart)

    def send_w(i, side, into):
        remote(w_ref.at[w_rows(0, i, side)], wall.at[w_rows(node * block, i, side)], y_peer, "w", into)

    def swap_w():
        here = wall.at[w_rows(other * block, 0, x)]
        received(here, "w0")
        remote(here, here, z_pair, "w", "w1")

    def relay_w(i):
        here = wall.at[w_rows(other * block, i, x)]
        if i > 0:
            received(here, f"w{i}")
        remote(here, here, x_peer, "wx", "wx")

    send_w(0, x, "w0")

    def both(i, first, other):
        pair = jnp.concatenate([first(p, i) for p in range(2)], axis=1)
        return mm_t(pair, other[...])

    def own_tok(p, i):
        return tok_ref[:, col(p, c, i)]

    def their_tok(p, i):
        return tokx[p, :, quarter_rows(p, i)]

    for i in range(4):
        acc[i] = both(i, own_tok, cot_ref)

    def chip_sum(i):
        if i == 0:
            received(cotx, "cot")
        received(tokx.at[0, :, pl.ds(0, 2 * quarter)], f"tok{i}")
        return acc[i] + both(i, their_tok, cotx)

    def cs(s):
        return slice(s * HD, (s + 1) * HD)

    def at(p, t):
        start = p * quarter + t % PIECES * rows_c
        return slice(start, start + rows_c), cs(t // PIECES)

    st1 = {}
    for i in range(2):
        value = chip_sum(i).astype(BF16)
        for t in range(chunks):
            for p in range(2):
                send1[i, p, t] = value[at(p, t)]
                st1[i, p, t] = copy_to(send1.at[i, p, t], recv1.at[i, p, t], towards[p][0], "first", f"first{i}{t}")
                if i == 0 or t < AHEAD:
                    st1[i, p, t].start()
    remote(w_ref, wall.at[own_w], partner, "wp", "wp")
    for i in range(2, 4):
        acc[i] = chip_sum(i)

    to_z, bcast, sg2, sg1 = {}, {}, {}, {}

    def second(t):
        received(recv1.at[0, :, t], f"first0{t}")
        for p in range(2):
            send2[p, t] = (acc[2][at(p, t)] + recv1[0, p, t].astype(F32)).astype(BF16)
            remote(send2.at[p, t], recv2.at[p, t], towards[p][1], "second", f"second{t}")
        if t + AHEAD < chunks:
            for p in range(2):
                st1[1, p, t + AHEAD].start()

    def to_root(t):
        h = t // PIECES
        received(recv1.at[1, :, t], f"first1{t}")
        received(recv2.at[:, t], f"second{t}")
        for p in range(2):
            rows, cols = at(p, t)
            total = acc[3, rows, cols] + recv1[1, p, t].astype(F32) + recv2[p, t].astype(F32)
            slot = lax.rem(z + 2 * zs - roots[p] - 1, zs)
            to_z[p, t] = copy_to(zsend.at[p, t], zrecv.at[t, slot], (node, roots[p] * 2 + x), f"z{p}", f"z{t}")

            @pl.when(z == roots[p])
            def _():
                acc[3, rows, cols] = total

            @pl.when(z != roots[p])
            def _():
                zsend[p, t] = total.astype(BF16)
                to_z[p, t].start()

            here = grad.at[p, h, chunk_rows(p, 3, t)]
            bcast[p, t] = [copy_to(here, here, (node, (roots[p] + d) % zs * 2 + x), "down", f"{('first1', 'second')[p]}{t}")
                           for d in range(1, zs)]
            sg1[p, t] = copy_to(here, here, towards[p][0], "gather", f"tok{t}")
            sg2[p, t] = copy_to(here, here, towards[p][1], "gather", f"first0{t}")

    def from_root(t):
        for p in range(2):
            @pl.when(z == roots[p])
            def _():
                rows, cols = at(p, t)
                total = acc[3, rows, cols]
                received(zrecv.at[t], f"z{t}")
                for d in range(zs - 1):
                    total = total + zrecv[t, d].astype(F32)
                grad[p, t // PIECES, chunk_rows(p, 3, t)] = total.astype(BF16)
                for cp in bcast[p, t]:
                    cp.start()
                sg2[p, t].start()
                sg1[p, t].start()

    def at_leaf(t):
        for p in range(2):
            @pl.when(z != roots[p])
            def _():
                bcast[p, t][0].wait_recv()
                sg2[p, t].start()
        for p in range(2):
            @pl.when(z != roots[p])
            def _():
                sg1[p, t].start()

    def last_gather(t):
        received(grad.at[:, 0, pl.ds(0, rows_c)], f"first0{t}")
        for p in range(2):
            there = grad.at[p, t // PIECES, chunk_rows(p, 2, t)]
            remote(there, there, towards[p][0], "gather", f"tok{t}")

    def input_rows(n, rows_of_w):
        rows = pl.ds(pl.multiple_of(n * block, block), block)
        out = lax.dot_general(cot_ref[...], rows_of_w, (((1,), (1,)), ((), ())), preferred_element_type=F32)
        igbuf[:, rows] = out.astype(BF16)

    def gathered(n):
        return wall[pl.ds(pl.multiple_of(n * block, block), block), :]

    def gram_of(h, p, bit):
        rows = pl.ds(pl.multiple_of(bit * half, half), half)
        g = grad[p, h, rows]
        return mm_t(g, g)

    for t in range(chunks):
        second(t)
        if t == SWAP_AT:
            swap_w()
    relay_w(0)
    send_w(2, x, "w2")
    send_w(3, x, "w3")
    send_w(3, 1 - x, "w3")
    input_rows(node, w_ref[...])
    received(w_ref, "wp")
    input_rows(y * 2 + 1 - c, gathered(y * 2 + 1 - c))

    def trade_w():
        received(wall.at[pl.ds(0, 3 * wpart)], "wx")
        received(wall.at[pl.ds(0, 2 * wpart)], "w3")
        y_w = pl.ds(pl.multiple_of(other * block, block), block)
        remote(wall.at[y_w], wall.at[y_w], partner, "wp", "wf")

    def finish_input():
        input_rows((1 - y) * 2 + c, gathered((1 - y) * 2 + c))
        received(w_ref, "wf")
        input_rows((1 - y) * 2 + 1 - c, gathered((1 - y) * 2 + 1 - c))

    def early_gram(s):
        early[s] = gram_of(s, 0, y) + gram_of(s, 1, x)

    def own_gram(s):
        for t in range(s * PIECES, (s + 1) * PIECES):
            received(grad.at[:, 0, pl.ds(0, 2 * rows_c)], f"tok{t}")
        gram_own[s] = early[s] + (gram_of(s, 0, 1 - y) + gram_of(s, 1, 1 - x))
        remote(gram_own.at[s], gram_in.at[s], partner, "gram", "gram")

    steps = {"z": to_root, "r": from_root, "l": at_leaf, "g": last_gather, "e": early_gram, "o": own_gram, "f": relay_w}
    extra = {"w": trade_w, "i": finish_input}
    for word in ORDER:
        if word in extra:
            extra[word]()
        else:
            steps[word[0]](int(word[1:]))

    rows_ref[...] = grad[y]
    received(gram_in, "gram")

    ii = lax.broadcasted_iota(jnp.int32, (HD, HD), 0)
    jj = lax.broadcasted_iota(jnp.int32, (HD, HD), 1)
    eye = (ii == jj).astype(F32)
    grams, totals, scales = [], [None] * heads, []
    for h in range(heads):
        raw = gram_own[h] + gram_in[h]
        squares = jnp.sum(jnp.sum(raw * eye, axis=1, keepdims=True), axis=0, keepdims=True)
        inverse = 1.0 / (jnp.sqrt(squares) + epsilon)
        scales.append(inverse)
        grams.append(raw * inverse * inverse)
    for step in range(NS_ITERS):
        rights = [right_form(g) for g in grams]
        squared = [product(left_form(g), r) for g, r in zip(grams, rights)]
        factors = [coef_a * eye + coef_b * g + coef_c * q for g, q in zip(grams, squared)]
        forms = [right_form(f) for f in factors]
        if step == 0:
            halfway = [product(left_form(g), f) for g, f in zip(grams, forms)]
        elif step + 1 < NS_ITERS:
            stacked = [jnp.concatenate([left_form(g), left_form(t)], axis=0) for g, t in zip(grams, totals)]
            pairs_of = [product(a, f) for a, f in zip(stacked, forms)]
            halfway, totals = [a[:HD] for a in pairs_of], [a[HD:] for a in pairs_of]
        if step == 0:
            totals = factors
        elif step + 1 == NS_ITERS:
            totals = [product(left_form(t), f) for t, f in zip(totals, forms)]
        if step + 1 < NS_ITERS:
            grams = [product(left_form(g), f) for g, f in zip(halfway, forms)]

    for h in range(heads):
        scaled = totals[h] * (scales[h] * (0.2 * math.sqrt(din)))
        form_ref[h] = jnp.concatenate(parts_of(scaled), axis=1)
    sent(cotx, "cot")
    sent(tokx, "tok")
    sent(send1, "first")
    sent(send2, "second")
    sent(wall.at[pl.ds(0, 5 * wpart)], "w")
    sent(wall.at[pl.ds(0, 3 * wpart)], "wx")
    sent(wall.at[pl.ds(0, 2 * block)], "wp")
    sent(grad.at[:, :, pl.ds(0, 3 * quarter)], "gather")
    sent(gram_own, "gram")
    for p in range(2):
        @pl.when(z == roots[p])
        def _():
            sent(grad.at[0, :, pl.ds(0, 3 * quarter)], "down")

        @pl.when(z != roots[p])
        def _():
            sent(zsend.at[p], f"z{p}")


def finish(ig_ref, rows_ref, form_ref, ig_out, up_out, upbuf, sems):
    heads = form_ref.shape[0]
    step = upbuf.shape[0] // 4
    copies = [pltpu.make_async_copy(ig_ref, ig_out, sems.at[0])]
    copies[0].start()
    for i in range(4):
        part = pl.ds(i * step, step)
        for h in range(heads):
            upbuf[part, pl.ds(h * HD, HD)] = product(rows_ref[h, part], form_ref[h])
        copies.append(pltpu.make_async_copy(upbuf.at[part], up_out.at[part], sems.at[i + 1]))
        copies[-1].start()
    for cp in copies:
        cp.wait()


def fused(tokens, cotangent, value_weight, zs):
    tok, din = tokens.shape
    width = cotangent.shape[1]
    heads = width // HD
    block = din // 4
    quarter = block // 4
    nsend = 12
    chunks, rows_c = heads * PIECES, quarter // PIECES
    nrecv = 1 + max(4, chunks) + 4 * chunks + WPARTS // 2 + 4
    vm, dma = pltpu.VMEM, pltpu.SemaphoreType.DMA
    held = pl.pallas_call(
        functools.partial(kernel, (width, heads, zs)),
        out_shape=(
            jax.ShapeDtypeStruct((tok, din), BF16),
            jax.ShapeDtypeStruct((heads, block, HD), BF16),
            jax.ShapeDtypeStruct((heads, HD, 2 * HD), BF16),
        ),
        in_specs=[pl.BlockSpec(memory_space=pl.ANY)] * 3,
        out_specs=(pl.BlockSpec(memory_space=pltpu.VMEM),) * 3,
        scratch_shapes=[
            vm((tok, din), BF16),
            vm((tok, width), BF16),
            vm((block, width), BF16),
            vm((2, tok, block), BF16),
            vm((tok, width), BF16),
            vm((din, width), BF16),
            vm((4, 2 * quarter, width), F32),
            vm((2, 2, chunks, rows_c, HD), BF16),
            vm((2, 2, chunks, rows_c, HD), BF16),
            vm((2, chunks, rows_c, HD), BF16),
            vm((2, chunks, rows_c, HD), BF16),
            vm((2, chunks, rows_c, HD), BF16),
            vm((chunks, zs - 1, rows_c, HD), BF16),
            vm((2, heads, block, HD), BF16),
            vm((heads, HD, HD), F32),
            vm((heads, HD, HD), F32),
            vm((heads, HD, HD), F32),
            dma((3,)),
            dma((nsend,)),
            dma((nrecv,)),
        ],
        compiler_params=pltpu.CompilerParams(collective_id=0, has_side_effects=True, vmem_limit_bytes=24 * 1024 * 1024),
    )(*(pltpu.with_memory_space_constraint(a, pltpu.HBM) for a in (tokens, cotangent, value_weight)))
    return pl.pallas_call(
        finish,
        out_shape=(jax.ShapeDtypeStruct((tok, din), BF16), jax.ShapeDtypeStruct((block, width), F32)),
        in_specs=[pl.BlockSpec(memory_space=pltpu.VMEM)] * 3,
        out_specs=(pl.BlockSpec(memory_space=pltpu.HBM),) * 2,
        scratch_shapes=[vm((block, width), F32), pltpu.SemaphoreType.DMA((5,))],
        compiler_params=pltpu.CompilerParams(vmem_limit_bytes=8 * 1024 * 1024),
    )(*held)


def general(tokens, cotangent, value_weight):
    width = value_weight.shape[1]
    din = tokens.shape[1]
    local_rows = value_weight.shape[0]
    heads = width // HD
    input_grad = lax.dot_general(
        cotangent,
        lax.all_gather(value_weight, "node", axis=0, tiled=True),
        (((1,), (1,)), ((), ())),
        preferred_element_type=F32,
    ).astype(BF16)
    partial_rows = lax.psum_scatter(
        lax.dot_general(tokens, cotangent, (((0,), (0,)), ((), ())), preferred_element_type=F32).astype(BF16),
        "node",
        scatter_dimension=0,
        tiled=True,
    ).astype(F32)
    gradient = lax.psum(partial_rows, "rep")
    blocks = gradient.reshape(local_rows, heads, HD)
    exact = functools.partial(jnp.einsum, precision=lax.Precision.HIGHEST)
    gram_raw = lax.psum(exact("rhi,rhj->hij", blocks, blocks), "node")
    divisor = jnp.sqrt(jnp.einsum("hii->h", gram_raw)) + epsilon
    gram = gram_raw / (divisor * divisor)[:, None, None]
    identity = jnp.broadcast_to(jnp.eye(HD, dtype=F32), (heads, HD, HD))
    total = identity
    for step in range(NS_ITERS):
        factor = coef_a * identity + coef_b * gram + coef_c * exact("hij,hjk->hik", gram, gram)
        total = exact("hij,hjk->hik", total, factor)
        if step + 1 < NS_ITERS:
            gram = exact("hji,hjk->hik", factor, exact("hij,hjk->hik", gram, factor))
    iterate = exact("rhi,hij->rhj", blocks / divisor[None, :, None], total)
    return input_grad, 0.2 * math.sqrt(din) * iterate.reshape(local_rows, width)


def solution(mesh):
    nodes, reps = mesh.shape["node"], mesh.shape["rep"]

    def per_device(tokens, cotangent, value_weight):
        zs = reps // 2
        fits = nodes == 4 and reps == 8 and tokens.shape[1] % (nodes * 4 * HD) == 0 and value_weight.shape[1] == 4 * HD
        if fits:
            return fused(tokens, cotangent, value_weight, zs)
        return general(tokens, cotangent, value_weight)

    return jax.shard_map(
        per_device,
        mesh=mesh,
        in_specs=(P(("node", "rep"), None), P(("node", "rep"), None), P("node", None)),
        out_specs=(P(("node", "rep"), None), P("node", None)),
        check_vma=False,
    )
```
